32 devices in a mesh: layer: 4 (over y, core), row: 4 (over z), col: 2 (over x).
Axes of the slice: x: 2, y: 2, z: 4, core: 2. Of those that a mesh axis runs over, the one named last changes fastest.
Arguments:
- left: float32 [2048, 1024], P('row', ('layer', 'col')), may hold values from -6 to 6
- right: float32 [1024, 32768], P(('layer', 'row'), 'col'), may hold values from -0.1875 to 0.1875
Outputs:
- product: float32 [2048, 32768], P(('row', 'layer'), 'col')
The draws below stay inside these ranges and needn't reach their ends.
All inputs are finite; a program needn't handle non-finite values.
Results may differ from the reference program's by a relative error of at most 0.000076.
Values sent between devices are 32-bit elements; how exact they have to be, the bound alone decides.
A program may use at most 128 MiB of HBM per device.

```python
import jax
import jax.numpy as jnp
from jax import lax

NCOLS = 32768
K = 1024
M = 2048


def block_scale(key, dims, cuts, low, top_value):
    loudness = 1.0
    for position, parts in cuts:
        steps = jax.random.uniform(jax.random.fold_in(jax.random.fold_in(key, 6), position), (parts,), jnp.float32, low / len(cuts), top_value / len(cuts))
        loudness = loudness * jnp.repeat(jnp.exp(steps), dims[position] // parts).reshape((-1,) + (1,) * (len(dims) - 1 - position))
    return loudness


def bell_draw(stream_key, dims, width, limit, split=(), dtype=jnp.bfloat16):
    array = width * jax.random.normal(stream_key, dims, jnp.float32)
    if split:
        array = array * block_scale(stream_key, dims, split, -0.22, 0.18)
    return jnp.clip(array, -limit, limit).astype(dtype)


def setup_inputs(seed: int = 0) -> dict:
    key_list = jax.random.split(jax.random.key(seed), 3)
    return {
        "left": bell_draw(key_list[0], (M, K), 1.0, 6.0, ((0, 4), (1, 8)), jnp.float32),
        "right": bell_draw(key_list[1], (K, NCOLS), K ** -0.5, 0.1875, ((0, 16), (1, 2)), jnp.float32),
    }


def reference(left, right):
    return jnp.dot(left, right, precision=lax.Precision.HIGHEST, preferred_element_type=jnp.float32)
```

```python
import functools

import jax
import jax.numpy as jnp
from jax import lax
from jax.experimental import pallas as pl
from jax.experimental.pallas import tpu as pltpu
from jax.sharding import PartitionSpec as P

MESH = pl.DeviceIdType.MESH
CORES = 2
AHEAD = 3
LEAD = 2
LEAD_OUTER = 6


def kernel(sizes, left, right, out, a_f32, a_hi, a_lo, b_all, b_hi, b_lo, c_buf,
           a1_s, a1_r, a2_s, a2_r, a3_s, a3_r, b1_s, b1_r, b2_s, b2_r, c_s, c_r, d_s, d_r):
    layers, rows, cols, chunks, width, tile = sizes
    half = rows // 2
    chips = layers // CORES
    l, z = lax.axis_index("layer"), lax.axis_index("row")
    x = lax.axis_index("col") if cols > 1 else 0
    y, c = l // CORES, l % CORES
    side = z // half
    base = side * half
    centre = half - 1 + side
    own = z - base
    piece = l * cols + x
    block = c_buf.shape[2] // layers
    is_centre = z == centre
    sibling = y * CORES + (1 - c)

    def remote(src, dst, send, recv, **to):
        return pltpu.make_async_remote_copy(
            src_ref=src, dst_ref=dst, send_sem=send, recv_sem=recv, device_id=to, device_id_type=MESH)

    barrier = pltpu.get_barrier_semaphore()
    greeted = 0
    for k in range(1, layers):
        pl.semaphore_signal(barrier, inc=1, device_id={"layer": lax.rem(l + k, layers)}, device_id_type=MESH)
        greeted += 1
    for k in range(1, rows):
        pl.semaphore_signal(barrier, inc=1, device_id={"row": lax.rem(z + k, rows)}, device_id_type=MESH)
        greeted += 1
    for k in range(1, cols):
        for m in range(chips):
            to = {"layer": lax.rem(l + m * CORES, layers), "col": lax.rem(x + k, cols)}
            pl.semaphore_signal(barrier, inc=1, device_id=to, device_id_type=MESH)
            greeted += 1
    pl.semaphore_wait(barrier, greeted)

    def b1(j, k):
        q = lax.rem(l + k, layers)
        src = right.at[:, pl.ds(pl.multiple_of((q * chunks + j) * width, width), width)]
        if k == 0:
            return pltpu.make_async_copy(src, b_all.at[j, l, z], b1_r.at[j, 0])
        return remote(src, b_all.at[j, l, z], b1_s.at[j, k], b1_r.at[j, k], layer=q)

    def b1_start(j):
        for k in range(layers):
            b1(j, k).start()

    def b1_wait(j):
        b1(j, 0).wait()
        for k in range(1, layers):
            b1(j, k).wait_recv()

    def b2(j, t):
        to = half - 1 + t
        return remote(b_all.at[j, :, z], b_all.at[j, :, z], b2_s.at[j, t], b2_r.at[j, z], row=to)

    def b2_start(j):
        for t in range(2):
            @pl.when(z != half - 1 + t)
            def _():
                b2(j, t).start()

    def b2_wait(j):
        for k in range(1, rows):
            src = lax.rem(z + k, rows)
            remote(b_all.at[j, :, src], b_all.at[j, :, src], b2_s.at[j, 0], b2_r.at[j, src], row=src).wait_recv()

    def gather_step(j):
        @pl.when(j + AHEAD < chunks)
        def _():
            b1_start(j + AHEAD)
        b1_wait(j)
        b2_start(j)

    def c_copy(j, s):
        return remote(c_buf.at[j, s], c_buf.at[j, s], c_s.at[j, s], c_r.at[j], row=base + s)

    def dist(j, k):
        q = lax.rem(l + k, layers)
        src = c_buf.at[j, own, pl.ds(pl.multiple_of(q * block, block), block)]
        dst = out.at[:, pl.ds(pl.multiple_of((l * chunks + j) * width, width), width)]
        if k == 0:
            return pltpu.make_async_copy(src, dst, d_r.at[j, 0])
        return remote(src, dst, d_s.at[j, k], d_r.at[j, k], layer=q)

    def dist_start(j):
        for k in range(1, layers):
            dist(j, k).start()
        dist(j, 0).start()

    def a1(s):
        return remote(left, a_f32.at[s, piece], a1_s, a1_r.at[s], row=centre)

    def a2(s, m, k, src):
        to = {"layer": lax.rem(l + m * CORES, layers)}
        if cols > 1:
            to["col"] = lax.rem(x + k, cols)
        return remote(src, a_f32.at[s, piece], a2_s.at[s, m, k], a2_r.at[s, m, k], **to)

    peers = [(m, k) for m in range(chips) for k in range(cols) if (m, k) != (0, 0)]

    def a3(s, m, k, core):
        ls = lax.rem(y + chips - m, chips) * CORES + core
        xs = lax.rem(x + cols - k, cols)
        p = ls * cols + xs
        return remote(a_f32.at[s, p], a_f32.at[s, p], a3_s.at[s, m, k], a3_r.at[s, m, k], layer=sibling)

    def local_a():
        return pltpu.make_async_copy(left, a_f32.at[own, piece], a1_r.at[own])

    def product(j):
        b = b_all[j].reshape(b_hi.shape)
        hi = b.astype(jnp.bfloat16)
        b_hi[...] = hi
        b_lo[...] = (b - hi.astype(jnp.float32)).astype(jnp.bfloat16)
        per = c_buf.shape[2] // tile
        for s in range(half):
            @pl.loop(0, per)
            def _(t):
                at = pl.ds(pl.multiple_of(t * tile, tile), tile)
                ah, al = a_hi[s, at, :], a_lo[s, at, :]
                dot = functools.partial(jnp.dot, preferred_element_type=jnp.float32)
                c_buf[j, s, at, :] = dot(al, b_hi[...]) + dot(ah, b_lo[...]) + dot(ah, b_hi[...])

    for j in range(min(AHEAD, chunks)):
        b1_start(j)
        if j == 0:
            @pl.when(jnp.logical_not(is_centre))
            def _():
                a1(own).start()

            @pl.when(is_centre)
            def _():
                local_a().start()
                for m, k in peers:
                    a2(own, m, k, left).start()

    lead = min(LEAD, chunks)
    lead_outer = min(LEAD_OUTER, chunks)

    @pl.when(is_centre)
    def _():
        @pl.loop(0, lead)
        def _(j):
            gather_step(j)
        local_a().wait()
        for i in range(1, half):
            s = lax.rem(own + i, half)
            a1(s).wait_recv()
            for m, k in peers:
                a2(s, m, k, a_f32.at[s, piece]).start()
        for i in range(half):
            s = lax.rem(own + i, half)
            a3(s, 0, 0, c).start()
            for m, k in peers:
                a2(s, m, k, left).wait_recv()
                a3(s, m, k, c).start()
        for i in range(half):
            s = lax.rem(own + i, half)
            for m, k in [(0, 0)] + peers:
                a3(s, m, k, 1 - c).wait_recv()
        wide = a_f32.shape[3]
        for s in range(half):
            for p in range(layers * cols):
                a = a_f32[s, p]
                hi = a.astype(jnp.bfloat16)
                a_hi[s, :, p * wide:(p + 1) * wide] = hi
                a_lo[s, :, p * wide:(p + 1) * wide] = (a - hi.astype(jnp.float32)).astype(jnp.bfloat16)

        @pl.loop(0, chunks)
        def _(j):
            @pl.when(j + lead < chunks)
            def _():
                gather_step(j + lead)
            b2_wait(j)
            product(j)
            for i in range(1, half):
                c_copy(j, lax.rem(own + i, half)).start()
            dist_start(j)

    @pl.when(jnp.logical_not(is_centre))
    def _():
        @pl.loop(0, lead_outer)
        def _(j):
            gather_step(j)

        @pl.loop(0, chunks)
        def _(j):
            @pl.when(j + lead_outer < chunks)
            def _():
                gather_step(j + lead_outer)
            c_copy(j, own).wait_recv()
            dist_start(j)

    @pl.loop(0, chunks)
    def _(j):
        dist(j, 0).wait()
        for k in range(1, layers):
            dist(j, k).wait()
            b1(j, k).wait_send()
        for t in range(2):
            @pl.when(z != half - 1 + t)
            def _():
                b2(j, t).wait_send()

        @pl.when(is_centre)
        def _():
            for i in range(1, half):
                c_copy(j, lax.rem(own + i, half)).wait_send()

    @pl.when(jnp.logical_not(is_centre))
    def _():
        a1(own).wait_send()

    @pl.when(is_centre)
    def _():
        for i in range(half):
            s = lax.rem(own + i, half)
            for m, k in peers:
                a2(s, m, k, left).wait_send()
            for m, k in [(0, 0)] + peers:
                a3(s, m, k, c).wait_send()


def body(mesh, left, right):
    layers, rows, cols = mesh.shape["layer"], mesh.shape["row"], mesh.shape["col"]
    if left.shape[1] % 128:
        left = lax.all_gather(left, "col", axis=1, tiled=True)
        cols = 1
    height, wide = left.shape
    depth, across = right.shape
    share = across // layers
    width = max(128, share // 16)
    chunks = share // width
    half = rows // 2
    inner = depth * layers * rows
    dma = pltpu.SemaphoreType.DMA
    sizes = (layers, rows, cols, chunks, width, min(256, height))
    chips = layers // CORES
    f32, bf16 = jnp.float32, jnp.bfloat16
    return pl.pallas_call(
        functools.partial(kernel, sizes),
        out_shape=jax.ShapeDtypeStruct((height // layers, across), f32),
        in_specs=[pl.BlockSpec(memory_space=pl.ANY)] * 2,
        out_specs=pl.BlockSpec(memory_space=pl.ANY),
        scratch_shapes=[
            pltpu.VMEM((half, layers * cols, height, wide), f32),
            pltpu.VMEM((half, height, inner), bf16),
            pltpu.VMEM((half, height, inner), bf16),
            pltpu.VMEM((chunks, layers, rows, depth, width), f32),
            pltpu.VMEM((inner, width), bf16),
            pltpu.VMEM((inner, width), bf16),
            pltpu.VMEM((chunks, half, height, width), f32),
            dma, dma((half,)),
            dma((half, chips, cols)), dma((half, chips, cols)),
            dma((half, chips, cols)), dma((half, chips, cols)),
            dma((chunks, layers)), dma((chunks, layers)),
            dma((chunks, 2)), dma((chunks, rows)),
            dma((chunks, half)), dma((chunks,)),
            dma((chunks, layers)), dma((chunks, layers)),
        ],
        compiler_params=pltpu.CompilerParams(
            collective_id=1, has_side_effects=True, vmem_limit_bytes=60 * 2**20),
    )(left, right)


def solution(mesh):
    in_specs = (P("row", ("layer", "col")), P(("layer", "row"), "col"))
    out_specs = P(("row", "layer"), "col")
    return jax.shard_map(
        functools.partial(body, mesh), mesh=mesh, in_specs=in_specs, out_specs=out_specs, check_vma=False)
```
